32 devices in a mesh: blk: 8 (over y, x, core), grp: 4 (over z).
Axes of the slice: x: 2, y: 2, z: 4, core: 2. Of those that a mesh axis runs over, the one named last changes fastest.
Arguments:
- queries: bfloat16 [8192, 4096], P(('blk', 'grp')), may hold values from -1 to 1
- documents: bfloat16 [8192, 4096], P(('blk', 'grp')), may hold values from -1 to 1
- positives: int32 [32, 256], P(('blk', 'grp')), may hold values from 0 to 255, as said below
Outputs:
- query_grad: float32 [8192, 4096], P(('blk', 'grp'))
- doc_grad: float32 [8192, 4096], P(('blk', 'grp'))
- loss: float32 [], replicated
The draws below stay inside these ranges and needn't reach their ends.
Inputs may be any that keep to these rules, and one draw needn't show every extreme that they name: `positives`: each block of 256 rows names each of 0 to 255 exactly once.
All inputs are finite; a program needn't handle non-finite values.
Results may differ from the reference program's by a relative error of at most 0.0036.
Values may be sent and summed in bfloat16 or wider, within the bound.
A program may use at most 128 MiB of HBM per device.

```python
import jax
import jax.numpy as jnp
from jax import lax

D = 4096
ROWS = 256
TOTAL = 8192
N_BLK = 8
N_GRP = 4


def common_draw(key):
    key_noise = jax.random.fold_in(key, 11)
    key_docs = jax.random.fold_in(key, 12)
    key_perm = jax.random.fold_in(key, 13)
    blocks = N_BLK * N_GRP
    perm_keys = jax.random.split(key_perm, blocks)
    positives = jax.vmap(lambda k: jax.random.permutation(k, ROWS))(perm_keys).astype(jnp.int32)
    docs = jax.random.normal(key_docs, (TOTAL, D), jnp.float32) * D ** (-0.5)
    noise = jax.random.normal(key_noise, (TOTAL, D), jnp.float32) * D ** (-0.5)
    span = 0.12
    rows = jnp.arange(TOTAL, dtype=jnp.int32)
    block = rows // ROWS
    shard = (block // N_GRP).astype(jnp.float32)
    align = span * shard / (N_BLK - 1)
    target = block * ROWS + positives.reshape(-1)
    paired = docs[target]
    raw_q = jnp.sqrt(1.0 - align * align)[:, None] * noise + align[:, None] * paired
    return (raw_q, docs, positives)


def draw_queries(key, part):
    return common_draw(key)[0].astype(jnp.bfloat16)


def draw_documents(key, part):
    return common_draw(key)[1].astype(jnp.bfloat16)


def draw_positives(key, part):
    return common_draw(key)[2]


def setup_inputs(seed: int = 0) -> dict:
    keys = jax.random.split(jax.random.key(seed), 4)
    queries = draw_queries(jax.random.fold_in(keys[3], 71), 0)
    documents = draw_documents(jax.random.fold_in(keys[3], 71), 0)
    positives = draw_positives(jax.random.fold_in(keys[3], 71), 0)
    return {"queries": queries, "documents": documents, "positives": positives}


SCALE = 50.0
EPSILON = 1e-06

def normalize(raw):
    wide = raw.astype(jnp.float32)
    ratio = lax.rsqrt(lax.optimization_barrier(jnp.sum(wide * wide, axis=-1, keepdims=True)) + EPSILON)
    return ((wide * ratio).astype(jnp.bfloat16), ratio)

def pull_back(grad, wide, ratio):
    inner = lax.optimization_barrier(jnp.sum(wide * grad, axis=-1, keepdims=True))
    return ratio * grad - ratio * ratio * ratio * inner * wide

def reference(queries, documents, positives):
    far = N_BLK // 4
    offsets = [0, 1, -1, far, -far]
    norm_q, ratio_q = normalize(queries)
    norm_d, ratio_d = normalize(documents)
    eq4 = norm_q.reshape(N_BLK, N_GRP, ROWS, D)
    ed4 = norm_d.reshape(N_BLK, N_GRP, ROWS, D)
    rq4 = ratio_q.reshape(N_BLK, N_GRP, ROWS, 1)
    rd4 = ratio_d.reshape(N_BLK, N_GRP, ROWS, 1)
    raw_q = queries.reshape(N_BLK, N_GRP, ROWS, D)
    raw_d = documents.reshape(N_BLK, N_GRP, ROWS, D)
    pos4 = positives.reshape(N_BLK, N_GRP, ROWS)
    columns = jnp.arange(ROWS, dtype=jnp.int32)

    def hot_of(index):
        return (columns[None, None, :] == pos4[index][:, :, None]).astype(jnp.float32)

    def forward(index):
        cand = jnp.stack([ed4[jnp.mod(index - off, N_BLK).astype(jnp.int32)] for off in offsets]).astype(jnp.float32)
        left = eq4[index].astype(jnp.float32)
        scores = SCALE * jnp.einsum('gid,cgjd->cgij', left, cand)
        lse = jnp.log(lax.optimization_barrier(jnp.sum(jnp.exp(scores), axis=(0, 3))))
        hot = hot_of(index)
        spos = lax.optimization_barrier(jnp.sum(scores[0] * hot, axis=-1))
        part = jnp.sum(lse - spos)
        probs = jnp.exp(scores - lse[None, :, :, None])
        probs = jnp.concatenate([(probs[0] - hot)[None], probs[1:]], axis=0)
        weights = probs.astype(jnp.bfloat16).astype(jnp.float32)
        direction = SCALE * jnp.einsum('cgij,cgjd->gid', weights, cand)
        grad = pull_back(direction, raw_q[index].astype(jnp.float32), rq4[index])
        return (grad, lse, part)
    grads_q, lses, parts = lax.map(forward, jnp.arange(N_BLK, dtype=jnp.int32))

    def backward(index):
        right = ed4[index].astype(jnp.float32)
        total = jnp.zeros((N_GRP, ROWS, D), jnp.float32)
        for off in offsets:
            source = jnp.mod(index + off, N_BLK).astype(jnp.int32)
            left = eq4[source].astype(jnp.float32)
            scores = SCALE * jnp.einsum('gid,gjd->gij', left, right)
            probs = jnp.exp(scores - lses[source][:, :, None])
            if off == 0:
                probs = probs - hot_of(index)
            weights = probs.astype(jnp.bfloat16).astype(jnp.float32)
            total = total + SCALE * jnp.einsum('gij,gid->gjd', weights, left)
        return pull_back(total, raw_d[index].astype(jnp.float32), rd4[index])
    grads_d = lax.map(backward, jnp.arange(N_BLK, dtype=jnp.int32))
    loss = jnp.sum(parts) / TOTAL
    return (grads_q.reshape(TOTAL, D), grads_d.reshape(TOTAL, D), loss)
```

```python
import jax
import jax.numpy as jnp
from jax import lax
from jax.sharding import PartitionSpec as P

SCALE = 50.0
EPSILON = 1e-06


def from_behind(value, axis, steps):
    count = lax.axis_size(axis)
    pairs = [(source, (source + steps) % count) for source in range(count)]
    return lax.ppermute(value, axis, pairs)


def normalize(raw):
    wide = raw.astype(jnp.float32)
    ratio = lax.rsqrt(jnp.sum(wide * wide, axis=-1, keepdims=True) + EPSILON)
    return ((wide * ratio).astype(jnp.bfloat16), wide, ratio)


def pull_back(grad, wide, ratio):
    inner = jnp.sum(wide * grad, axis=-1, keepdims=True)
    return ratio * grad - ratio * ratio * ratio * inner * wide


def score_block(left, right):
    return SCALE * jnp.einsum("id,jd->ij", left, right, preferred_element_type=jnp.float32)


def transpose_product(weights, left):
    return SCALE * jnp.einsum("ij,id->jd", weights, left, preferred_element_type=jnp.float32)


def on_device_plain(queries, documents, positives):
    norm_q, wide_q, ratio_q = normalize(queries)
    norm_d, wide_d, ratio_d = normalize(documents)
    width = lax.axis_size("blk")
    far = width // 4
    offsets = [1, -1, far, -far]
    rows = norm_q.shape[0]
    received = [norm_d]
    for off in offsets:
        received.append(from_behind(norm_d, "blk", off))
    scores = [score_block(norm_q, block) for block in received]
    total = scores[0].shape[0] * 0.0 + jnp.zeros((rows,), jnp.float32)
    for block_scores in scores:
        total = total + jnp.sum(jnp.exp(block_scores), axis=-1)
    lse = jnp.log(total)
    columns = jnp.arange(rows, dtype=jnp.int32)
    hot = (columns[None, :] == positives[0][:, None]).astype(jnp.float32)
    spos = jnp.sum(scores[0] * hot, axis=-1)
    part = jnp.sum(lse - spos)
    weights = [(jnp.exp(scores[0] - lse[:, None]) - hot).astype(jnp.bfloat16)]
    for block_scores in scores[1:]:
        weights.append(jnp.exp(block_scores - lse[:, None]).astype(jnp.bfloat16))
    query_dir = jnp.zeros_like(wide_q)
    for weight, block in zip(weights, received):
        query_dir = query_dir + SCALE * jnp.dot(weight, block, preferred_element_type=jnp.float32)
    doc_dir = transpose_product(weights[0], norm_q)
    for off, weight in zip(offsets, weights[1:]):
        partial_grad = transpose_product(weight, norm_q)
        doc_dir = doc_dir + from_behind(partial_grad.astype(jnp.bfloat16), "blk", -off).astype(
            partial_grad.dtype
        )
    query_grad = pull_back(query_dir, wide_q, ratio_q)
    doc_grad = pull_back(doc_dir, wide_d, ratio_d)
    summed = lax.psum(part, ("blk", "grp"))
    loss = summed / (rows * width * lax.axis_size("grp"))
    return (query_grad, doc_grad, loss)

CORES = 2
CHUNKS = 4


def flip(value, bit):
    count = lax.axis_size("blk")
    return lax.ppermute(value, "blk", [(source, source ^ bit) for source in range(count)])


def on_device_relay(queries, documents, positives):
    norm_q, wide_q, ratio_q = normalize(queries)
    norm_d, wide_d, ratio_d = normalize(documents)
    rows = norm_q.shape[0]
    step = rows // CHUNKS
    index = lax.axis_index("blk")
    relay_near = (index & 1) == ((index >> 1) & 1)
    cuts = [slice(c * step, (c + 1) * step) for c in range(CHUNKS)]
    near = [flip(norm_d[cut], 2) for cut in cuts]
    sibling_d = flip(norm_d, 1)
    sibling_q = flip(norm_q, 1)
    diag = [flip(block, 4) for block in near]
    relayed = [flip(jnp.where(relay_near, n, g), 1) for n, g in zip(near, diag)]
    own_scores = score_block(norm_q, norm_d)
    sib_scores = score_block(norm_q, sibling_d)

    def chunked(blocks):
        return jnp.concatenate([score_block(norm_q, b) for b in blocks], axis=1)

    scores = [own_scores, sib_scores, chunked(near), chunked(diag), chunked(relayed)]
    total = jnp.zeros((rows,), jnp.float32)
    for block_scores in scores:
        total = total + jnp.sum(jnp.exp(block_scores), axis=-1)
    lse = jnp.log(total)
    columns = jnp.arange(rows, dtype=jnp.int32)
    hot = (columns[None, :] == positives[0][:, None]).astype(jnp.float32)
    spos = jnp.sum(own_scores * hot, axis=-1)
    part = jnp.sum(lse - spos)
    w_own = (jnp.exp(own_scores - lse[:, None]) - hot).astype(jnp.bfloat16)
    w_sib, w_near, w_diag, w_rel = [
        jnp.exp(b - lse[:, None]).astype(jnp.bfloat16) for b in scores[1:]
    ]
    swapped = flip(jnp.concatenate([w_sib, w_rel], axis=1), 1)
    v_own, v_rel = swapped[:, :rows], swapped[:, rows:]
    zero = jnp.zeros_like(v_rel)
    both_q = jnp.concatenate([norm_q, sibling_q], axis=0)
    to_diag = jnp.concatenate([w_diag, jnp.where(relay_near, zero, v_rel)], axis=0)
    to_near = jnp.concatenate([w_near, jnp.where(relay_near, v_rel, zero)], axis=0)
    to_own = jnp.concatenate([w_own, v_own], axis=0)
    far_sums = [
        flip(transpose_product(to_diag[:, cut], both_q).astype(jnp.bfloat16), 4) for cut in cuts
    ]
    sums = []
    for cut, arrived in zip(cuts, far_sums):
        term = transpose_product(to_near[:, cut], both_q) + arrived.astype(jnp.float32)
        sums.append(flip(term.astype(jnp.bfloat16), 2))
    weights = jnp.concatenate([w_own, w_sib, w_near, w_diag, w_rel], axis=1)
    blocks = jnp.concatenate([norm_d, sibling_d] + near + diag + relayed, axis=0)
    query_dir = SCALE * jnp.dot(weights, blocks, preferred_element_type=jnp.float32)
    query_grad = pull_back(query_dir, wide_q, ratio_q)
    doc_own = transpose_product(to_own, both_q)
    doc_dir = doc_own + jnp.concatenate(sums, axis=0).astype(jnp.float32)
    doc_grad = pull_back(doc_dir, wide_d, ratio_d)
    summed = lax.psum(part, ("blk", "grp"))
    loss = summed / (rows * lax.axis_size("blk") * lax.axis_size("grp"))
    return (query_grad, doc_grad, loss)


def on_device(queries, documents, positives):
    if lax.axis_size("blk") // 4 == CORES:
        return on_device_relay(queries, documents, positives)
    return on_device_plain(queries, documents, positives)


def solution(mesh):
    return jax.shard_map(
        on_device,
        mesh=mesh,
        in_specs=(P(("blk", "grp"), None), P(("blk", "grp"), None), P(("blk", "grp"), None)),
        out_specs=(P(("blk", "grp"), None), P(("blk", "grp"), None), P()),
        check_vma=False,
    )
```

```python
import jax
import jax.numpy as jnp
from jax import lax
from jax.sharding import PartitionSpec as P

SCALE = 50.0
EPSILON = 1e-06


def from_behind(value, axis, steps):
    count = lax.axis_size(axis)
    pairs = [(source, (source + steps) % count) for source in range(count)]
    return lax.ppermute(value, axis, pairs)


def normalize(raw):
    wide = raw.astype(jnp.float32)
    ratio = lax.rsqrt(jnp.sum(wide * wide, axis=-1, keepdims=True) + EPSILON)
    return ((wide * ratio).astype(jnp.bfloat16), wide, ratio)


def pull_back(grad, wide, ratio):
    inner = jnp.sum(wide * grad, axis=-1, keepdims=True)
    return ratio * grad - ratio * ratio * ratio * inner * wide


def score_block(left, right):
    return SCALE * jnp.einsum("id,jd->ij", left, right, preferred_element_type=jnp.float32)


def transpose_product(weights, left):
    return SCALE * jnp.einsum("ij,id->jd", weights, left, preferred_element_type=jnp.float32)


def on_device_plain(queries, documents, positives):
    norm_q, wide_q, ratio_q = normalize(queries)
    norm_d, wide_d, ratio_d = normalize(documents)
    width = lax.axis_size("blk")
    far = width // 4
    offsets = [1, -1, far, -far]
    rows = norm_q.shape[0]
    received = [norm_d]
    for off in offsets:
        received.append(from_behind(norm_d, "blk", off))
    scores = [score_block(norm_q, block) for block in received]
    total = scores[0].shape[0] * 0.0 + jnp.zeros((rows,), jnp.float32)
    for block_scores in scores:
        total = total + jnp.sum(jnp.exp(block_scores), axis=-1)
    lse = jnp.log(total)
    columns = jnp.arange(rows, dtype=jnp.int32)
    hot = (columns[None, :] == positives[0][:, None]).astype(jnp.float32)
    spos = jnp.sum(scores[0] * hot, axis=-1)
    part = jnp.sum(lse - spos)
    weights = [(jnp.exp(scores[0] - lse[:, None]) - hot).astype(jnp.bfloat16)]
    for block_scores in scores[1:]:
        weights.append(jnp.exp(block_scores - lse[:, None]).astype(jnp.bfloat16))
    query_dir = jnp.zeros_like(wide_q)
    for weight, block in zip(weights, received):
        query_dir = query_dir + SCALE * jnp.dot(weight, block, preferred_element_type=jnp.float32)
    doc_dir = transpose_product(weights[0], norm_q)
    for off, weight in zip(offsets, weights[1:]):
        partial_grad = transpose_product(weight, norm_q)
        doc_dir = doc_dir + from_behind(partial_grad.astype(jnp.bfloat16), "blk", -off).astype(
            partial_grad.dtype
        )
    query_grad = pull_back(query_dir, wide_q, ratio_q)
    doc_grad = pull_back(doc_dir, wide_d, ratio_d)
    summed = lax.psum(part, ("blk", "grp"))
    loss = summed / (rows * width * lax.axis_size("grp"))
    return (query_grad, doc_grad, loss)


CORES = 2
CHUNKS = 4


def flip(value, bit):
    count = lax.axis_size("blk")
    return lax.ppermute(value, "blk", [(source, source ^ bit) for source in range(count)])


def total_of(part):
    value = jnp.full((8, 128), part)
    for axis in ("blk", "grp"):
        count = lax.axis_size(axis)
        if count & (count - 1):
            value = lax.psum(value, axis)
            continue
        bit = count // 2
        while bit:
            value = value + lax.ppermute(value, axis, [(n, n ^ bit) for n in range(count)])
            bit //= 2
    return value[0, 0]


def after(value, *others):
    return lax.optimization_barrier((value, *others))[0]


def on_device_relay(queries, documents, positives):
    rows = queries.shape[0]
    step = rows // CHUNKS
    index = lax.axis_index("blk")
    relay_near = (index & 1) == ((index >> 1) & 1)
    cuts = [slice(c * step, (c + 1) * step) for c in range(CHUNKS)]
    raw_near = []
    for c, cut in enumerate(cuts):
        piece = documents[cut]
        if c >= 2:
            piece = after(piece, raw_near[c - 2])
        raw_near.append(flip(piece, 2))
    raw_sibling_d = flip(documents, 1)
    raw_sibling_q = flip(queries, 1)
    raw_diag = []
    for block in raw_near:
        raw_diag.append(flip(block, 4))
    raw_relayed = [flip(jnp.where(relay_near, n, g), 1) for n, g in zip(raw_near, raw_diag)]
    norm_q, wide_q, ratio_q = normalize(queries)
    norm_d, wide_d, ratio_d = normalize(documents)
    sibling_d = normalize(raw_sibling_d)[0]
    sibling_q = normalize(raw_sibling_q)[0]
    near, diag, relayed = [
        [normalize(block)[0] for block in blocks] for blocks in (raw_near, raw_diag, raw_relayed)
    ]
    own_scores = score_block(norm_q, norm_d)
    sib_scores = score_block(norm_q, sibling_d)

    def chunked(blocks):
        return jnp.concatenate([score_block(norm_q, b) for b in blocks], axis=1)

    scores = [own_scores, sib_scores, chunked(near), chunked(diag), chunked(relayed)]
    total = jnp.zeros((rows,), jnp.float32)
    for block_scores in scores:
        total = total + jnp.sum(jnp.exp(block_scores), axis=-1)
    lse = jnp.log(total)
    columns = jnp.arange(rows, dtype=jnp.int32)
    hot = (columns[None, :] == positives[0][:, None]).astype(jnp.float32)
    spos = jnp.sum(own_scores * hot, axis=-1)
    part = jnp.sum(lse - spos)
    w_own = (jnp.exp(own_scores - lse[:, None]) - hot).astype(jnp.bfloat16)
    w_sib, w_near, w_diag, w_rel = [
        jnp.exp(b - lse[:, None]).astype(jnp.bfloat16) for b in scores[1:]
    ]
    swapped = flip(jnp.concatenate([w_sib, w_rel], axis=1), 1)
    v_own, v_rel = swapped[:, :rows], swapped[:, rows:]
    zero = jnp.zeros_like(v_rel)
    both_q = jnp.concatenate([norm_q, sibling_q], axis=0)
    to_diag = jnp.concatenate([w_diag, jnp.where(relay_near, zero, v_rel)], axis=0)
    to_near = jnp.concatenate([w_near, jnp.where(relay_near, v_rel, zero)], axis=0)
    to_own = jnp.concatenate([w_own, v_own], axis=0)
    far_sums = []
    for c, cut in enumerate(cuts):
        weight = to_diag[:, cut]
        if c >= 2:
            weight = after(weight, far_sums[c - 2])
        term = transpose_product(weight, both_q).astype(jnp.bfloat16)
        far_sums.append(flip(term, 4))
    groups = [([w_own, w_sib], [norm_d, sibling_d]), ([w_near], near), ([w_diag], diag), ([w_rel], relayed)]
    query_dir = jnp.zeros(queries.shape, jnp.float32)
    sums = []
    for c, cut in enumerate(cuts):
        arrived = far_sums[c] if c == 0 else after(far_sums[c], term)
        term = transpose_product(to_near[:, cut], both_q) + arrived.astype(jnp.float32)
        term = term.astype(jnp.bfloat16)
        sums.append(flip(term, 2))
        for weight, blocks in groups[c * len(groups) // CHUNKS : (c + 1) * len(groups) // CHUNKS]:
            weight, blocks, _ = lax.optimization_barrier((weight, blocks, term))
            query_dir = query_dir + SCALE * jnp.dot(
                jnp.concatenate(weight, axis=1),
                jnp.concatenate(blocks, axis=0),
                preferred_element_type=jnp.float32,
            )
        if c == 1:
            to_own = after(to_own, term)
    query_grad = pull_back(query_dir, wide_q, ratio_q)
    doc_own = transpose_product(to_own, both_q)
    doc_dir = doc_own + jnp.concatenate(sums, axis=0).astype(jnp.float32)
    doc_grad = pull_back(doc_dir, wide_d, ratio_d)
    summed = total_of(part)
    loss = summed / (rows * lax.axis_size("blk") * lax.axis_size("grp"))
    return (query_grad, doc_grad, loss)


def on_device(queries, documents, positives):
    if lax.axis_size("blk") // 4 == CORES:
        return on_device_relay(queries, documents, positives)
    return on_device_plain(queries, documents, positives)


def solution(mesh):
    return jax.shard_map(
        on_device,
        mesh=mesh,
        in_specs=(P(("blk", "grp"), None), P(("blk", "grp"), None), P(("blk", "grp"), None)),
        out_specs=(P(("blk", "grp"), None), P(("blk", "grp"), None), P()),
        check_vma=False,
    )
```
